32 devices in a mesh: leaf: 4 (over z), row: 2 (over x), col: 4 (over y, core).
Axes of the slice: x: 2, y: 2, z: 4, core: 2. Of those that a mesh axis runs over, the one named last changes fastest.
Arguments:
- pivot: float32 [4, 1024, 1024], P('leaf', 'row', 'col'), as said below
- border: float32 [4, 3072, 1024], P('leaf', 'row', 'col'), may hold values from -0.065625 to 0.065625
- update: float32 [4, 3072, 3072], P('leaf', 'row', 'col'), as said below
- child_map: int32 [4, 3072], replicated, may hold values from 0 to 4607, as said below
- parent_diag: float32 [4, 2304], P('leaf', 'row'), may hold values from 0.5 to 4
Outputs:
- factor_pivot: float32 [4, 1024, 1024], P('leaf', 'row', 'col')
- factor_border: float32 [4, 3072, 1024], P('leaf', 'row', 'col')
- parent_front: float32 [4, 2304, 4608], P('leaf', 'row', 'col')
The draws below stay inside these ranges and needn't reach their ends.
Inputs may be any that keep to these rules, and one draw needn't show every extreme that they name: Each row child_map[l] is increasing with distinct entries, and its i-th block of 768 entries lies among parent rows i * 1152 to (i+1) * 1152 - 1. Each pivot[l] is symmetric positive definite. Each update[l] is symmetric.
All inputs are finite; a program needn't handle non-finite values.
Results may differ from the reference program's by a relative error of at most 0.00007.
Values sent between devices are 32-bit elements; how exact they have to be, the bound alone decides.
A program may use at most 128 MiB of HBM per device.

```python
import math
import jax
import jax.numpy as jnp
from jax import lax

PANEL = 1024
UPD = 3072
PARENT = 4608
CHILD = 4096
LEAVES = 4
NB = 4
RB = 1152
N_ROW = 2


def symmetric_part(key, count, order):
    noise = jax.random.normal(key, (count, order, order), jnp.float32)
    return (noise + jnp.swapaxes(noise, 1, 2)) * (0.7 / math.sqrt(2.0 * CHILD))


def dominant(key, order):
    first, second = jax.random.split(key)
    diagonal = jax.random.uniform(second, (LEAVES, order), jnp.float32, 2.0, 4.0)
    return symmetric_part(first, LEAVES, order) + diagonal[:, :, None] * jnp.eye(order, dtype=jnp.float32)[None]


def coupling(key, order):
    places = jnp.arange(order, dtype=jnp.float32)
    distance = jnp.abs(places[:, None] - places[None, :])
    kernel = (3.0 + 6.0 * jnp.exp(-distance * (4.0 / order))) / order
    strength = jax.random.uniform(key, (LEAVES,), jnp.float32, 0.8, 1.6)
    return strength[:, None, None] * kernel[None]


def draw_pivot(key, part):
    base = dominant(jax.random.fold_in(key, 11), PANEL)
    return base + coupling(jax.random.fold_in(key, 19), PANEL)


def draw_update(key, part):
    return dominant(jax.random.fold_in(key, 13), UPD)


def draw_child_map(key, part):
    keys = jax.random.split(jax.random.fold_in(key, 17), LEAVES * NB)

    def choose(single):
        return jnp.sort(jax.random.permutation(single, PARENT // NB)[:UPD // NB])
    picked = jax.vmap(choose)(keys).reshape(LEAVES, NB, UPD // NB)
    offsets = (jnp.arange(NB, dtype=jnp.int32) * (PARENT // NB))[None, :, None]
    return (picked.astype(jnp.int32) + offsets).reshape(LEAVES, UPD).astype(jnp.int32)


def block_scale(key, extent, cuts, least, largest):
    gain = 1.0
    for dim, blocks in cuts:
        heights = jax.random.uniform(jax.random.fold_in(jax.random.fold_in(key, 6), dim), (blocks,), jnp.float32, least / len(cuts), largest / len(cuts))
        gain = gain * jnp.repeat(jnp.exp(heights), extent[dim] // blocks).reshape((-1,) + (1,) * (len(extent) - 1 - dim))
    return gain


def bell_draw(key, shape, spread, bound, cuts=(), held_as=jnp.bfloat16):
    array = jax.random.normal(key, shape, jnp.float32) * spread
    if len(cuts) > 0:
        array = block_scale(key, shape, cuts, -0.22, 0.18) * array
    return jnp.clip(array, min=-bound, max=bound).astype(held_as)


def setup_inputs(seed: int = 0) -> dict:
    splits = jax.random.split(jax.random.key(seed), 6)
    return {
        "pivot": draw_pivot(jax.random.fold_in(splits[5], 71), 0),
        "border": bell_draw(splits[1], (LEAVES, UPD, PANEL), (0.7 / (CHILD ** 0.5)), 0.065625, ((0, 4), (1, 2), (2, 4)), jnp.float32),
        "update": draw_update(jax.random.fold_in(splits[5], 71), 0),
        "child_map": draw_child_map(jax.random.fold_in(splits[5], 71), 0),
        "parent_diag": jnp.clip(jnp.exp(math.log(4.0) - 2.0794415 * jax.random.uniform(splits[4], (LEAVES, PARENT // 2), jnp.float32) ** block_scale(splits[4], (LEAVES, PARENT // 2), ((0, 4), (1, 2)), -0.2, 0.2)), 0.5, 4.0),
    }


def eliminate(blocks):
    piv, bord, upd = blocks
    lower = jnp.linalg.cholesky(piv)
    below = lax.linalg.triangular_solve(lower, bord, left_side=False, lower=True, transpose_a=True)
    schur = upd - jnp.dot(below.astype(jnp.float32), below.T.astype(jnp.float32), precision=lax.Precision.HIGHEST, preferred_element_type=jnp.float32)
    return (lower, below, schur)

def reference(pivot, border, update, child_map, parent_diag):
    lowers, belows, schurs = lax.map(eliminate, (pivot, border, update))
    fronts = []
    for pair in range(LEAVES // 2):
        front = jnp.zeros((PARENT, PARENT), jnp.float32)
        for side in range(2):
            index = child_map[2 * pair + side]
            front = front.at[index[:, None], index[None, :]].add(schurs[2 * pair + side])
        diag_rows = parent_diag[2 * pair:2 * pair + 2].reshape(2, N_ROW, RB).transpose(1, 0, 2).reshape(PARENT)
        front = front + jnp.diag(diag_rows)
        fronts.append(front.reshape(N_ROW, 2, RB, PARENT).transpose(1, 0, 2, 3).reshape(2, PARENT // 2, PARENT))
    return (lowers, belows, jnp.concatenate(fronts, axis=0))
```

```python
import jax
import jax.numpy as jnp
from jax import lax
from jax.experimental import pallas as pl
from jax.experimental.pallas import tpu as pltpu
from jax.sharding import PartitionSpec as P

BLOCK = 128
PANEL = 8
HIGH = lax.Precision.HIGH


def exact_dot(left, right):
    return jnp.dot(left, right, precision=lax.Precision.HIGHEST, preferred_element_type=jnp.float32)


def factor_small(entry):
    work = {key: value for key, value in entry.items()}
    lower = {}
    inverse = {}
    for k in range(PANEL):
        scale = lax.rsqrt(work[k, k])
        for i in range(k + 1, PANEL):
            lower[i, k] = work[i, k] * scale
        for j in range(k + 1, PANEL):
            for i in range(j, PANEL):
                work[i, j] = work[i, j] - lower[i, k] * lower[j, k]
        inverse[k, k] = scale
        for j in range(k):
            total = lower[k, j] * inverse[j, j]
            for m in range(j + 1, k):
                total = total + lower[k, m] * inverse[m, j]
            inverse[k, j] = -(total * scale)
    return inverse


def factor_block(diag, upper, inv):
    lane8 = lax.broadcasted_iota(jnp.int32, (PANEL, BLOCK), 1)
    lane_all = lax.broadcasted_iota(jnp.int32, (BLOCK, BLOCK), 1)

    def panel_step(p, carry):
        base = p * PANEL
        start = pl.multiple_of(base, PANEL)
        rows = diag[pl.ds(start, PANEL), :]
        full = diag[...]
        entry = {}
        for b in range(PANEL):
            index = jnp.zeros((PANEL, BLOCK), jnp.int32) + (base + b)
            col = jnp.take_along_axis(rows, index, axis=1, mode="promise_in_bounds")
            for a in range(b, PANEL):
                entry[a, b] = jnp.broadcast_to(col[a : a + 1, :], (PANEL, BLOCK))
        inverse = factor_small(entry)
        inside = (lane8 >= base) & (lane8 < base + PANEL)
        plain = []
        augmented = []
        for k in range(PANEL):
            row = jnp.broadcast_to(rows[k : k + 1, :], (PANEL, BLOCK))
            plain.append(row)
            augmented.append(jnp.where(inside, (lane8 == base + k).astype(jnp.float32), row))
        solved = []
        for a in range(PANEL):
            up = inverse[a, 0] * plain[0]
            au = inverse[a, 0] * augmented[0]
            for k in range(1, a + 1):
                up = up + inverse[a, k] * plain[k]
                au = au + inverse[a, k] * augmented[k]
            solved.append(au)
            keep = lane8 >= base + a
            upper[pl.ds(start + a, 1), :] = jnp.where(keep, up, 0.0)[0:1, :]
            inv[pl.ds(start + a, 1), :] = jnp.where(lane8 <= base + a, au, 0.0)[0:1, :]
        inside_all = (lane_all >= base) & (lane_all < base + PANEL)
        trailing = jnp.where(inside_all, 0.0, full)
        for m in range(PANEL):
            gain = inverse[m, m] * solved[m]
            for a in range(m + 1, PANEL):
                gain = gain + inverse[a, m] * solved[a]
            index = jnp.zeros((BLOCK, BLOCK), jnp.int32) + (base + m)
            col = jnp.take_along_axis(full, index, axis=1, mode="promise_in_bounds")
            trailing = trailing - col * jnp.broadcast_to(gain[0:1, :], (BLOCK, BLOCK))
        diag[...] = trailing
        return carry

    lax.fori_loop(0, BLOCK // PANEL, panel_step, 0)


def factor_kernel(pivot, upper_out, inverse_out, work, diag, upper, inv, panel):
    order = pivot.shape[0]
    count = order // BLOCK
    lane = lax.broadcasted_iota(jnp.int32, (BLOCK, order), 1)
    work[...] = pivot[...]

    def block_step(kb, carry):
        start = pl.multiple_of(kb * BLOCK, BLOCK)
        here = pl.ds(start, BLOCK)
        diag[...] = work[here, here]
        factor_block(diag, upper, inv)
        work[here, here] = jnp.where(
            lax.broadcasted_iota(jnp.int32, (BLOCK, BLOCK), 0)
            == lax.broadcasted_iota(jnp.int32, (BLOCK, BLOCK), 1),
            1.0,
            0.0,
        )
        panel[...] = exact_dot(inv[...], work[here, :])
        solved = panel[...]
        inverse_out[here, :] = jnp.where(lane < start + BLOCK, solved, 0.0)
        upper_out[here, :] = jnp.where(lane >= start + BLOCK, solved, 0.0)
        upper_out[here, here] = upper[...]

        def row_step(ib, carry):
            there = pl.ds(pl.multiple_of(ib * BLOCK, BLOCK), BLOCK)
            left = panel[:, there].T
            work[there, here] = jnp.zeros((BLOCK, BLOCK), jnp.float32)
            work[there, :] = work[there, :] - exact_dot(left, panel[...])
            return carry

        lax.fori_loop(kb + 1, count, row_step, 0)
        return carry

    lax.fori_loop(0, count, block_step, 0)


def factor(pivot):
    order = pivot.shape[0]
    spec = pl.BlockSpec(memory_space=pltpu.VMEM)
    shape = jax.ShapeDtypeStruct((order, order), jnp.float32)
    return pl.pallas_call(
        factor_kernel,
        out_shape=(shape, shape),
        in_specs=[spec],
        out_specs=(spec, spec),
        scratch_shapes=[
            pltpu.VMEM((order, order), jnp.float32),
            pltpu.VMEM((BLOCK, BLOCK), jnp.float32),
            pltpu.VMEM((BLOCK, BLOCK), jnp.float32),
            pltpu.VMEM((BLOCK, BLOCK), jnp.float32),
            pltpu.VMEM((BLOCK, order), jnp.float32),
        ],
        compiler_params=pltpu.CompilerParams(vmem_limit_bytes=40 * 2**20),
        cost_estimate=pl.CostEstimate(
            flops=60 * order**3, bytes_accessed=12 * order * order, transcendentals=order
        ),
        name="factor",
    )(pivot)


def high_dot_t(left, right):
    return lax.dot_general(
        left, right, (((1,), (1,)), ((), ())), precision=HIGH, preferred_element_type=jnp.float32
    )


def split_two(value):
    top = lax.reduce_precision(value, 8, 7)
    return top.astype(jnp.bfloat16), (value - top).astype(jnp.bfloat16)


def one_hot(targets, size):
    return (jnp.arange(size, dtype=jnp.int32)[:, None] == targets[None, :]).astype(jnp.bfloat16)


def pick_dot(left, right, dims):
    return lax.dot_general(left, right, (dims, ((), ())), preferred_element_type=jnp.float32)


def place_block(block, rows_to, cols_to, out_rows, out_cols):
    col_hot = one_hot(cols_to, out_cols)
    row_hot = one_hot(rows_to, out_rows)
    top, rest = split_two(block)
    wide = pick_dot(top, col_hot, ((1,), (1,))) + pick_dot(rest, col_hot, ((1,), (1,)))
    top, rest = split_two(wide)
    return pick_dot(row_hot, top, ((1,), (0,))) + pick_dot(row_hot, rest, ((1,), (0,)))


def column_border(full_rows, nrow, ncol, cols_local, row_index, col_index):
    rows_local = full_rows.shape[0]
    if rows_local % cols_local == 0 and rows_local > cols_local:
        per_row = rows_local // cols_local
        mine = lax.dynamic_slice_in_dim(full_rows, (col_index % per_row) * cols_local, cols_local, 0)
        result = mine
        for shift in range(1, nrow):
            pairs = []
            for c in range(ncol):
                source = c // per_row
                target = (source + shift) % nrow
                pairs.append((source * ncol + c, target * ncol + c))
            moved = lax.ppermute(mine, ("row", "col"), pairs)
            hit = row_index == (col_index // per_row + shift) % nrow
            result = jnp.where(hit, moved, result)
        return result
    whole = lax.all_gather(full_rows, "row", axis=0, tiled=True)
    return lax.dynamic_slice_in_dim(whole, col_index * cols_local, cols_local, 0)


def on_device(pivot, border, update, child_map, parent_diag):
    nrow = lax.axis_size("row")
    ncol = lax.axis_size("col")
    row_index = lax.axis_index("row")
    col_index = lax.axis_index("col")
    leaf_index = lax.axis_index("leaf")
    piece = pivot[0]
    piece_rows, piece_cols = piece.shape
    stacked = lax.all_gather(piece[None], ("row", "col"), axis=0, tiled=True)
    whole = (
        stacked.reshape(nrow, ncol, piece_rows, piece_cols)
        .transpose(0, 2, 1, 3)
        .reshape(nrow * piece_rows, ncol * piece_cols)
    )
    upper, inverse = factor(whole)
    pivot_out = lax.dynamic_slice(
        upper, (col_index * piece_cols, row_index * piece_rows), (piece_cols, piece_rows)
    ).T

    bord = border[0]
    rows_local = bord.shape[0]
    trailing = update[0]
    cols_local = trailing.shape[1]
    full_rows = lax.all_gather(bord, "col", axis=1, tiled=True)
    col_rows = column_border(full_rows, nrow, ncol, cols_local, row_index, col_index)
    factor_cols = high_dot_t(col_rows, inverse)

    half_rows = parent_diag.shape[1]
    block_rows = 2 * half_rows
    parent_cols = block_rows * nrow // ncol
    side = leaf_index % 2
    partner = leaf_index + 1 - 2 * side
    total_cols = child_map.shape[1]
    own_map = lax.dynamic_slice(child_map, (leaf_index, 0), (1, total_cols))[0]
    partner_map = lax.dynamic_slice(child_map, (partner, 0), (1, total_cols))[0]
    swap = [(source, source ^ 1) for source in range(lax.axis_size("leaf"))]

    map_block = total_cols // max(nrow, ncol)
    halves = rows_local % (2 * map_block) == 0
    if halves:
        kept = rows_local // 2
        own_start = side * kept
        sent_start = (1 - side) * kept

        def schur_rows(start):
            rows = lax.dynamic_slice_in_dim(full_rows, start, kept, 0)
            below = high_dot_t(rows, inverse)
            part = lax.dynamic_slice_in_dim(trailing, start, kept, 0)
            return below, part - high_dot_t(below, factor_cols)

        sent_below, sent = schur_rows(sent_start)
        sibling = lax.ppermute(sent, "leaf", swap)
        own_below, own = schur_rows(own_start)
        own_slice = lax.dynamic_slice_in_dim(own_below, col_index * piece_cols, piece_cols, 1)
        sent_slice = lax.dynamic_slice_in_dim(sent_below, col_index * piece_cols, piece_cols, 1)
        border_out = jnp.where(
            side == 0,
            jnp.concatenate([own_slice, sent_slice], axis=0),
            jnp.concatenate([sent_slice, own_slice], axis=0),
        )
    else:
        kept = rows_local
        own_start = 0
        factor_rows = high_dot_t(full_rows, inverse)
        own = trailing - high_dot_t(factor_rows, factor_cols)
        sibling = lax.ppermute(own, "leaf", swap)
        border_out = lax.dynamic_slice_in_dim(factor_rows, col_index * piece_cols, piece_cols, 1)

    def my_half(block, mapping):
        rows_to = (
            lax.dynamic_slice_in_dim(mapping, row_index * rows_local + own_start, kept)
            - row_index * block_rows
            - side * half_rows
        )
        cols_to = (
            lax.dynamic_slice_in_dim(mapping, col_index * cols_local, cols_local)
            - col_index * parent_cols
        )
        return place_block(block, rows_to, cols_to, half_rows, parent_cols)

    global_rows = row_index * block_rows + side * half_rows + jnp.arange(half_rows, dtype=jnp.int32)
    global_cols = col_index * parent_cols + jnp.arange(parent_cols, dtype=jnp.int32)
    diagonal = jnp.where(global_rows[:, None] == global_cols[None, :], parent_diag[0][:, None], 0.0)
    parent_out = my_half(own, own_map) + diagonal + my_half(sibling, partner_map)
    return (pivot_out[None], border_out[None], parent_out[None])


def solution(mesh):
    placed = (
        P("leaf", "row", "col"),
        P("leaf", "row", "col"),
        P("leaf", "row", "col"),
        P(),
        P("leaf", "row"),
    )
    return jax.shard_map(
        on_device,
        mesh=mesh,
        in_specs=placed,
        out_specs=(P("leaf", "row", "col"), P("leaf", "row", "col"), P("leaf", "row", "col")),
        check_vma=False,
    )
```

```python
import jax
import jax.numpy as jnp
from jax import lax
from jax.experimental import pallas as pl
from jax.experimental.pallas import tpu as pltpu
from jax.sharding import PartitionSpec as P

BLOCK = 128
CHUNKS = 2
PANEL = 8
HIGH = lax.Precision.HIGH


def exact_dot(left, right):
    return jnp.dot(left, right, precision=lax.Precision.HIGHEST, preferred_element_type=jnp.float32)


def factor_small(entry):
    work = {key: value for key, value in entry.items()}
    lower = {}
    inverse = {}
    for k in range(PANEL):
        scale = lax.rsqrt(work[k, k])
        for i in range(k + 1, PANEL):
            lower[i, k] = work[i, k] * scale
        for j in range(k + 1, PANEL):
            for i in range(j, PANEL):
                work[i, j] = work[i, j] - lower[i, k] * lower[j, k]
        inverse[k, k] = scale
        for j in range(k):
            total = lower[k, j] * inverse[j, j]
            for m in range(j + 1, k):
                total = total + lower[k, m] * inverse[m, j]
            inverse[k, j] = -(total * scale)
    return inverse


def factor_block(diag, upper, inv):
    lane8 = lax.broadcasted_iota(jnp.int32, (PANEL, BLOCK), 1)
    lane_all = lax.broadcasted_iota(jnp.int32, (BLOCK, BLOCK), 1)

    def panel_step(p, carry):
        base = p * PANEL
        start = pl.multiple_of(base, PANEL)
        rows = diag[pl.ds(start, PANEL), :]
        full = diag[...]
        entry = {}
        for b in range(PANEL):
            index = jnp.zeros((PANEL, BLOCK), jnp.int32) + (base + b)
            col = jnp.take_along_axis(rows, index, axis=1, mode="promise_in_bounds")
            for a in range(b, PANEL):
                entry[a, b] = jnp.broadcast_to(col[a : a + 1, :], (PANEL, BLOCK))
        inverse = factor_small(entry)
        inside = (lane8 >= base) & (lane8 < base + PANEL)
        plain = []
        augmented = []
        for k in range(PANEL):
            row = jnp.broadcast_to(rows[k : k + 1, :], (PANEL, BLOCK))
            plain.append(row)
            augmented.append(jnp.where(inside, (lane8 == base + k).astype(jnp.float32), row))
        solved = []
        for a in range(PANEL):
            up = inverse[a, 0] * plain[0]
            au = inverse[a, 0] * augmented[0]
            for k in range(1, a + 1):
                up = up + inverse[a, k] * plain[k]
                au = au + inverse[a, k] * augmented[k]
            solved.append(au)
            keep = lane8 >= base + a
            upper[pl.ds(start + a, 1), :] = jnp.where(keep, up, 0.0)[0:1, :]
            inv[pl.ds(start + a, 1), :] = jnp.where(lane8 <= base + a, au, 0.0)[0:1, :]
        inside_all = (lane_all >= base) & (lane_all < base + PANEL)
        trailing = jnp.where(inside_all, 0.0, full)
        for m in range(PANEL):
            gain = inverse[m, m] * solved[m]
            for a in range(m + 1, PANEL):
                gain = gain + inverse[a, m] * solved[a]
            index = jnp.zeros((BLOCK, BLOCK), jnp.int32) + (base + m)
            col = jnp.take_along_axis(full, index, axis=1, mode="promise_in_bounds")
            trailing = trailing - col * jnp.broadcast_to(gain[0:1, :], (BLOCK, BLOCK))
        diag[...] = trailing
        return carry

    lax.fori_loop(0, BLOCK // PANEL, panel_step, 0)


def factor_kernel(pivot, upper_out, inverse_out, work, diag, upper, inv, panel):
    order = work.shape[0]
    count = order // BLOCK
    lane = lax.broadcasted_iota(jnp.int32, (BLOCK, order), 1)
    pieces, piece_rows, piece_cols = pivot.shape
    across = order // piece_cols
    for index in range(pieces):
        first_row = index // across * piece_rows
        first_col = index % across * piece_cols
        if first_row < first_col + piece_cols:
            work[pl.ds(first_row, piece_rows), pl.ds(first_col, piece_cols)] = pivot[index]
        else:
            work[pl.ds(first_row, piece_rows), pl.ds(first_col, piece_cols)] = jnp.zeros(
                (piece_rows, piece_cols), jnp.float32
            )

    def block_step(kb, carry):
        start = pl.multiple_of(kb * BLOCK, BLOCK)
        here = pl.ds(start, BLOCK)
        diag[...] = work[here, here]
        factor_block(diag, upper, inv)
        work[here, here] = jnp.where(
            lax.broadcasted_iota(jnp.int32, (BLOCK, BLOCK), 0)
            == lax.broadcasted_iota(jnp.int32, (BLOCK, BLOCK), 1),
            1.0,
            0.0,
        )
        panel[...] = exact_dot(inv[...], work[here, :])
        solved = panel[...]
        inverse_out[here, :] = jnp.where(lane < start + BLOCK, solved, 0.0)
        upper_out[here, :] = jnp.where(lane >= start + BLOCK, solved, 0.0)
        upper_out[here, here] = upper[...]

        def row_step(ib, carry):
            there = pl.ds(pl.multiple_of(ib * BLOCK, BLOCK), BLOCK)
            left = panel[:, there].T
            work[there, here] = jnp.zeros((BLOCK, BLOCK), jnp.float32)
            work[there, :] = work[there, :] - exact_dot(left, panel[...])
            return carry

        lax.fori_loop(kb + 1, count, row_step, 0)
        return carry

    lax.fori_loop(0, count, block_step, 0)


def factor(pivot, order):
    spec = pl.BlockSpec(memory_space=pltpu.VMEM)
    shape = jax.ShapeDtypeStruct((order, order), jnp.float32)
    return pl.pallas_call(
        factor_kernel,
        out_shape=(shape, shape),
        in_specs=[spec],
        out_specs=(spec, spec),
        scratch_shapes=[
            pltpu.VMEM((order, order), jnp.float32),
            pltpu.VMEM((BLOCK, BLOCK), jnp.float32),
            pltpu.VMEM((BLOCK, BLOCK), jnp.float32),
            pltpu.VMEM((BLOCK, BLOCK), jnp.float32),
            pltpu.VMEM((BLOCK, order), jnp.float32),
        ],
        compiler_params=pltpu.CompilerParams(vmem_limit_bytes=40 * 2**20),
        cost_estimate=pl.CostEstimate(
            flops=60 * order**3, bytes_accessed=12 * order * order, transcendentals=order
        ),
        name="factor",
    )(pivot)


def high_dot_t(left, right):
    return lax.dot_general(
        left, right, (((1,), (1,)), ((), ())), precision=HIGH, preferred_element_type=jnp.float32
    )


def split_two(value):
    top = lax.reduce_precision(value, 8, 7)
    return top.astype(jnp.bfloat16), (value - top).astype(jnp.bfloat16)


def one_hot(targets, size):
    return (jnp.arange(size, dtype=jnp.int32)[:, None] == targets[None, :]).astype(jnp.bfloat16)


def pick_dot(left, right, dims):
    return lax.dot_general(left, right, (dims, ((), ())), preferred_element_type=jnp.float32)


def place_blocks(blocks, rows_to, cols_to, out_rows, out_cols):
    col_hot = one_hot(cols_to, out_cols)
    first = 0
    placed = None
    for block in blocks:
        count = block.shape[0]
        row_hot = one_hot(rows_to[first : first + count], out_rows)
        first += count
        top, rest = split_two(block)
        wide = pick_dot(top, col_hot, ((1,), (1,))) + pick_dot(rest, col_hot, ((1,), (1,)))
        top, rest = split_two(wide)
        part = pick_dot(row_hot, top, ((1,), (0,))) + pick_dot(row_hot, rest, ((1,), (0,)))
        placed = part if placed is None else placed + part
    return placed


def column_border(bord, full_rows, nrow, ncol, cols_local, row_index, col_index):
    rows_local, width = bord.shape
    if nrow == 2 and rows_local % cols_local == 0:
        per_row = rows_local // cols_local
        mine = lax.dynamic_slice_in_dim(full_rows, (col_index % per_row) * cols_local, cols_local, 0)
        received = jnp.zeros((cols_local, full_rows.shape[1]), bord.dtype)
        for shift in range(ncol):
            pairs = []
            for c in range(ncol):
                home = c // per_row
                pairs.append((home * ncol + (c + shift) % ncol, (1 - home) * ncol + c))
            target = (col_index - shift + ncol) % ncol
            part = lax.dynamic_slice_in_dim(bord, (target % per_row) * cols_local, cols_local, 0)
            moved = lax.ppermute(part, ("row", "col"), pairs)
            place = (col_index + shift) % ncol * width
            received = lax.dynamic_update_slice_in_dim(received, moved, place, 1)
        return jnp.where(row_index == col_index // per_row, mine, received)
    whole = lax.all_gather(full_rows, "row", axis=0, tiled=True)
    return lax.dynamic_slice_in_dim(whole, col_index * cols_local, cols_local, 0)


def on_device(pivot, border, update, child_map, parent_diag):
    nrow = lax.axis_size("row")
    ncol = lax.axis_size("col")
    row_index = lax.axis_index("row")
    col_index = lax.axis_index("col")
    leaf_index = lax.axis_index("leaf")
    piece = pivot[0]
    piece_rows, piece_cols = piece.shape
    stacked = lax.all_gather(piece[None], ("row", "col"), axis=0, tiled=True)
    stacked, bord = lax.optimization_barrier((stacked, border[0]))
    upper, inverse = factor(stacked, nrow * piece_rows)
    pivot_out = lax.dynamic_slice(
        upper, (col_index * piece_cols, row_index * piece_rows), (piece_cols, piece_rows)
    ).T

    rows_local = bord.shape[0]
    trailing = update[0]
    cols_local = trailing.shape[1]
    full_rows = lax.all_gather(bord, "col", axis=1, tiled=True)
    col_rows = column_border(bord, full_rows, nrow, ncol, cols_local, row_index, col_index)
    factor_cols = high_dot_t(col_rows, inverse)

    half_rows = parent_diag.shape[1]
    block_rows = 2 * half_rows
    parent_cols = block_rows * nrow // ncol
    side = leaf_index % 2
    partner = leaf_index + 1 - 2 * side
    total_cols = child_map.shape[1]
    own_map = lax.dynamic_slice(child_map, (leaf_index, 0), (1, total_cols))[0]
    partner_map = lax.dynamic_slice(child_map, (partner, 0), (1, total_cols))[0]
    swap = [(source, source ^ 1) for source in range(lax.axis_size("leaf"))]

    map_block = total_cols // max(nrow, ncol)
    halves = rows_local % (2 * map_block) == 0
    if halves:
        kept = rows_local // 2
        own_start = side * kept
        sent_start = (1 - side) * kept

        def schur_rows(start, size):
            rows = lax.dynamic_slice_in_dim(full_rows, start, size, 0)
            below = high_dot_t(rows, inverse)
            part = lax.dynamic_slice_in_dim(trailing, start, size, 0)
            return below, part - high_dot_t(below, factor_cols)

        sent_parts = []
        sibling = []
        chunk = kept // CHUNKS
        for index in range(CHUNKS):
            below, sent = schur_rows(sent_start + index * chunk, chunk)
            sent_parts.append(below)
            sibling.append(lax.ppermute(sent, "leaf", swap))
        sent_below = jnp.concatenate(sent_parts, axis=0)
        own_below, own = schur_rows(own_start, kept)
        own_slice = lax.dynamic_slice_in_dim(own_below, col_index * piece_cols, piece_cols, 1)
        sent_slice = lax.dynamic_slice_in_dim(sent_below, col_index * piece_cols, piece_cols, 1)
        border_out = jnp.where(
            side == 0,
            jnp.concatenate([own_slice, sent_slice], axis=0),
            jnp.concatenate([sent_slice, own_slice], axis=0),
        )
    else:
        kept = rows_local
        own_start = 0
        factor_rows = high_dot_t(full_rows, inverse)
        own = trailing - high_dot_t(factor_rows, factor_cols)
        sibling = [lax.ppermute(own, "leaf", swap)]
        border_out = lax.dynamic_slice_in_dim(factor_rows, col_index * piece_cols, piece_cols, 1)

    def my_half(blocks, mapping):
        rows_to = (
            lax.dynamic_slice_in_dim(mapping, row_index * rows_local + own_start, kept)
            - row_index * block_rows
            - side * half_rows
        )
        cols_to = (
            lax.dynamic_slice_in_dim(mapping, col_index * cols_local, cols_local)
            - col_index * parent_cols
        )
        return place_blocks(blocks, rows_to, cols_to, half_rows, parent_cols)

    global_rows = row_index * block_rows + side * half_rows + jnp.arange(half_rows, dtype=jnp.int32)
    global_cols = col_index * parent_cols + jnp.arange(parent_cols, dtype=jnp.int32)
    diagonal = jnp.where(global_rows[:, None] == global_cols[None, :], parent_diag[0][:, None], 0.0)
    parent_out = my_half([own], own_map) + diagonal + my_half(sibling, partner_map)
    return (pivot_out[None], border_out[None], parent_out[None])


def solution(mesh):
    placed = (
        P("leaf", "row", "col"),
        P("leaf", "row", "col"),
        P("leaf", "row", "col"),
        P(),
        P("leaf", "row"),
    )
    return jax.shard_map(
        on_device,
        mesh=mesh,
        in_specs=placed,
        out_specs=(P("leaf", "row", "col"), P("leaf", "row", "col"), P("leaf", "row", "col")),
        check_vma=False,
    )
```

```python
import jax
import jax.numpy as jnp
from jax import lax
from jax.experimental import pallas as pl
from jax.experimental.pallas import tpu as pltpu
from jax.sharding import PartitionSpec as P

BLOCK = 128
CHUNKS = 2
PANEL = 8
HIGH = lax.Precision.HIGH


def exact_dot(left, right):
    return jnp.dot(left, right, precision=lax.Precision.HIGHEST, preferred_element_type=jnp.float32)


def factor_small(entry):
    work = {key: value for key, value in entry.items()}
    lower = {}
    inverse = {}
    for k in range(PANEL):
        scale = lax.rsqrt(work[k, k])
        for i in range(k + 1, PANEL):
            lower[i, k] = work[i, k] * scale
        for j in range(k + 1, PANEL):
            for i in range(j, PANEL):
                work[i, j] = work[i, j] - lower[i, k] * lower[j, k]
        inverse[k, k] = scale
        for j in range(k):
            total = lower[k, j] * inverse[j, j]
            for m in range(j + 1, k):
                total = total + lower[k, m] * inverse[m, j]
            inverse[k, j] = -(total * scale)
    return inverse


def factor_block(diag, upper, inv):
    lane8 = lax.broadcasted_iota(jnp.int32, (PANEL, BLOCK), 1)
    lane_all = lax.broadcasted_iota(jnp.int32, (BLOCK, BLOCK), 1)

    def panel_step(p, carry):
        base = p * PANEL
        start = pl.multiple_of(base, PANEL)
        rows = diag[pl.ds(start, PANEL), :]
        full = diag[...]
        entry = {}
        for b in range(PANEL):
            index = jnp.zeros((PANEL, BLOCK), jnp.int32) + (base + b)
            col = jnp.take_along_axis(rows, index, axis=1, mode="promise_in_bounds")
            for a in range(b, PANEL):
                entry[a, b] = jnp.broadcast_to(col[a : a + 1, :], (PANEL, BLOCK))
        inverse = factor_small(entry)
        inside = (lane8 >= base) & (lane8 < base + PANEL)
        plain = []
        augmented = []
        for k in range(PANEL):
            row = jnp.broadcast_to(rows[k : k + 1, :], (PANEL, BLOCK))
            plain.append(row)
            augmented.append(jnp.where(inside, (lane8 == base + k).astype(jnp.float32), row))
        solved = []
        for a in range(PANEL):
            up = inverse[a, 0] * plain[0]
            au = inverse[a, 0] * augmented[0]
            for k in range(1, a + 1):
                up = up + inverse[a, k] * plain[k]
                au = au + inverse[a, k] * augmented[k]
            solved.append(au)
            keep = lane8 >= base + a
            upper[pl.ds(start + a, 1), :] = jnp.where(keep, up, 0.0)[0:1, :]
            inv[pl.ds(start + a, 1), :] = jnp.where(lane8 <= base + a, au, 0.0)[0:1, :]
        inside_all = (lane_all >= base) & (lane_all < base + PANEL)
        trailing = jnp.where(inside_all, 0.0, full)
        for m in range(PANEL):
            gain = inverse[m, m] * solved[m]
            for a in range(m + 1, PANEL):
                gain = gain + inverse[a, m] * solved[a]
            index = jnp.zeros((BLOCK, BLOCK), jnp.int32) + (base + m)
            col = jnp.take_along_axis(full, index, axis=1, mode="promise_in_bounds")
            trailing = trailing - col * jnp.broadcast_to(gain[0:1, :], (BLOCK, BLOCK))
        diag[...] = trailing
        return carry

    lax.fori_loop(0, BLOCK // PANEL, panel_step, 0)


def split_three(value):
    top = value.astype(jnp.bfloat16)
    rest = value - top.astype(jnp.float32)
    mid = rest.astype(jnp.bfloat16)
    return top, mid, (rest - mid.astype(jnp.float32)).astype(jnp.bfloat16)


def factor_kernel(pivot, upper_out, inverse_out, work, diag, upper, inv, panel, parts):
    order = work.shape[0]
    count = order // BLOCK
    lane = lax.broadcasted_iota(jnp.int32, (BLOCK, order), 1)
    pieces, piece_rows, piece_cols = pivot.shape
    across = order // piece_cols
    for index in range(pieces):
        first_row = index // across * piece_rows
        first_col = index % across * piece_cols
        if first_row < first_col + piece_cols:
            work[pl.ds(first_row, piece_rows), pl.ds(first_col, piece_cols)] = pivot[index]
        else:
            work[pl.ds(first_row, piece_rows), pl.ds(first_col, piece_cols)] = jnp.zeros(
                (piece_rows, piece_cols), jnp.float32
            )

    def block_step(kb, carry):
        start = pl.multiple_of(kb * BLOCK, BLOCK)
        here = pl.ds(start, BLOCK)
        diag[...] = work[here, here]
        factor_block(diag, upper, inv)
        work[here, here] = jnp.where(
            lax.broadcasted_iota(jnp.int32, (BLOCK, BLOCK), 0)
            == lax.broadcasted_iota(jnp.int32, (BLOCK, BLOCK), 1),
            1.0,
            0.0,
        )
        panel[...] = exact_dot(inv[...], work[here, :])
        solved = panel[...]
        inverse_out[here, :] = jnp.where(lane < start + BLOCK, solved, 0.0)
        upper_out[here, :] = jnp.where(lane >= start + BLOCK, solved, 0.0)
        upper_out[here, here] = upper[...]

        top, mid, low = split_three(solved)
        parts[0, :BLOCK, :] = top
        parts[0, BLOCK:, :] = top
        parts[1, :BLOCK, :] = mid
        parts[1, BLOCK:, :] = mid
        parts[2, :BLOCK, :] = low
        parts[2, BLOCK:, :] = top

        def row_step(ib, carry):
            there = pl.ds(pl.multiple_of(ib * BLOCK, BLOCK), BLOCK)
            top, mid, low = split_three(panel[:, there].T)
            both = jnp.concatenate([top, mid], axis=1)
            ends = jnp.concatenate([top, low], axis=1)
            change = jnp.dot(ends, parts[2], preferred_element_type=jnp.float32)
            change = change + jnp.dot(both, parts[1], preferred_element_type=jnp.float32)
            change = change + jnp.dot(both, parts[0], preferred_element_type=jnp.float32)
            work[there, here] = jnp.zeros((BLOCK, BLOCK), jnp.float32)
            work[there, :] = work[there, :] - change
            return carry

        lax.fori_loop(kb + 1, count, row_step, 0)
        return carry

    lax.fori_loop(0, count, block_step, 0)


def factor(pivot, order):
    spec = pl.BlockSpec(memory_space=pltpu.VMEM)
    shape = jax.ShapeDtypeStruct((order, order), jnp.float32)
    return pl.pallas_call(
        factor_kernel,
        out_shape=(shape, shape),
        in_specs=[spec],
        out_specs=(spec, spec),
        scratch_shapes=[
            pltpu.VMEM((order, order), jnp.float32),
            pltpu.VMEM((BLOCK, BLOCK), jnp.float32),
            pltpu.VMEM((BLOCK, BLOCK), jnp.float32),
            pltpu.VMEM((BLOCK, BLOCK), jnp.float32),
            pltpu.VMEM((BLOCK, order), jnp.float32),
            pltpu.VMEM((3, 2 * BLOCK, order), jnp.bfloat16),
        ],
        compiler_params=pltpu.CompilerParams(vmem_limit_bytes=40 * 2**20),
        cost_estimate=pl.CostEstimate(
            flops=60 * order**3, bytes_accessed=12 * order * order, transcendentals=order
        ),
        name="factor",
    )(pivot)


def high_dot_t(left, right):
    return lax.dot_general(
        left, right, (((1,), (1,)), ((), ())), precision=HIGH, preferred_element_type=jnp.float32
    )


def split_two(value):
    top = lax.reduce_precision(value, 8, 7)
    return top.astype(jnp.bfloat16), (value - top).astype(jnp.bfloat16)


def one_hot(targets, size):
    return (jnp.arange(size, dtype=jnp.int32)[:, None] == targets[None, :]).astype(jnp.bfloat16)


def pick_dot(left, right, dims):
    return lax.dot_general(left, right, (dims, ((), ())), preferred_element_type=jnp.float32)


def place_blocks(blocks, rows_to, cols_to, out_rows, out_cols):
    col_hot = one_hot(cols_to, out_cols)
    first = 0
    placed = None
    for block in blocks:
        count = block.shape[0]
        row_hot = one_hot(rows_to[first : first + count], out_rows)
        first += count
        top, rest = split_two(block)
        wide = pick_dot(top, col_hot, ((1,), (1,))) + pick_dot(rest, col_hot, ((1,), (1,)))
        top, rest = split_two(wide)
        part = pick_dot(row_hot, top, ((1,), (0,))) + pick_dot(row_hot, rest, ((1,), (0,)))
        placed = part if placed is None else placed + part
    return placed


def column_border(bord, full_rows, nrow, ncol, cols_local, row_index, col_index):
    rows_local, width = bord.shape
    if nrow == 2 and rows_local % cols_local == 0:
        per_row = rows_local // cols_local
        mine = lax.dynamic_slice_in_dim(full_rows, (col_index % per_row) * cols_local, cols_local, 0)
        received = jnp.zeros((cols_local, full_rows.shape[1]), bord.dtype)
        for shift in range(ncol):
            pairs = []
            for c in range(ncol):
                home = c // per_row
                pairs.append((home * ncol + (c + shift) % ncol, (1 - home) * ncol + c))
            target = (col_index - shift + ncol) % ncol
            part = lax.dynamic_slice_in_dim(bord, (target % per_row) * cols_local, cols_local, 0)
            moved = lax.ppermute(part, ("row", "col"), pairs)
            place = (col_index + shift) % ncol * width
            received = lax.dynamic_update_slice_in_dim(received, moved, place, 1)
        return jnp.where(row_index == col_index // per_row, mine, received)
    whole = lax.all_gather(full_rows, "row", axis=0, tiled=True)
    return lax.dynamic_slice_in_dim(whole, col_index * cols_local, cols_local, 0)


def on_device(pivot, border, update, child_map, parent_diag):
    nrow = lax.axis_size("row")
    ncol = lax.axis_size("col")
    row_index = lax.axis_index("row")
    col_index = lax.axis_index("col")
    leaf_index = lax.axis_index("leaf")
    piece = pivot[0]
    piece_rows, piece_cols = piece.shape
    stacked = lax.all_gather(piece[None], ("row", "col"), axis=0, tiled=True)
    stacked, bord = lax.optimization_barrier((stacked, border[0]))
    upper, inverse = factor(stacked, nrow * piece_rows)
    pivot_out = lax.dynamic_slice(
        upper, (col_index * piece_cols, row_index * piece_rows), (piece_cols, piece_rows)
    ).T

    rows_local = bord.shape[0]
    trailing = update[0]
    cols_local = trailing.shape[1]
    full_rows = lax.all_gather(bord, "col", axis=1, tiled=True)
    col_rows = column_border(bord, full_rows, nrow, ncol, cols_local, row_index, col_index)
    factor_cols = high_dot_t(col_rows, inverse)

    half_rows = parent_diag.shape[1]
    block_rows = 2 * half_rows
    parent_cols = block_rows * nrow // ncol
    side = leaf_index % 2
    partner = leaf_index + 1 - 2 * side
    total_cols = child_map.shape[1]
    own_map = lax.dynamic_slice(child_map, (leaf_index, 0), (1, total_cols))[0]
    partner_map = lax.dynamic_slice(child_map, (partner, 0), (1, total_cols))[0]
    swap = [(source, source ^ 1) for source in range(lax.axis_size("leaf"))]

    map_block = total_cols // max(nrow, ncol)
    halves = rows_local % (2 * map_block) == 0
    if halves:
        kept = rows_local // 2
        own_start = side * kept
        sent_start = (1 - side) * kept

        def schur_rows(start, size):
            rows = lax.dynamic_slice_in_dim(full_rows, start, size, 0)
            below = high_dot_t(rows, inverse)
            part = lax.dynamic_slice_in_dim(trailing, start, size, 0)
            return below, part - high_dot_t(below, factor_cols)

        sent_parts = []
        sibling = []
        chunk = kept // CHUNKS
        for index in range(CHUNKS):
            below, sent = schur_rows(sent_start + index * chunk, chunk)
            sent_parts.append(below)
            sibling.append(lax.ppermute(sent, "leaf", swap))
        sent_below = jnp.concatenate(sent_parts, axis=0)
        own_below, own = schur_rows(own_start, kept)
        own_slice = lax.dynamic_slice_in_dim(own_below, col_index * piece_cols, piece_cols, 1)
        sent_slice = lax.dynamic_slice_in_dim(sent_below, col_index * piece_cols, piece_cols, 1)
        border_out = jnp.where(
            side == 0,
            jnp.concatenate([own_slice, sent_slice], axis=0),
            jnp.concatenate([sent_slice, own_slice], axis=0),
        )
    else:
        kept = rows_local
        own_start = 0
        factor_rows = high_dot_t(full_rows, inverse)
        own = trailing - high_dot_t(factor_rows, factor_cols)
        sibling = [lax.ppermute(own, "leaf", swap)]
        border_out = lax.dynamic_slice_in_dim(factor_rows, col_index * piece_cols, piece_cols, 1)

    def my_half(blocks, mapping):
        rows_to = (
            lax.dynamic_slice_in_dim(mapping, row_index * rows_local + own_start, kept)
            - row_index * block_rows
            - side * half_rows
        )
        cols_to = (
            lax.dynamic_slice_in_dim(mapping, col_index * cols_local, cols_local)
            - col_index * parent_cols
        )
        return place_blocks(blocks, rows_to, cols_to, half_rows, parent_cols)

    global_rows = row_index * block_rows + side * half_rows + jnp.arange(half_rows, dtype=jnp.int32)
    global_cols = col_index * parent_cols + jnp.arange(parent_cols, dtype=jnp.int32)
    diagonal = jnp.where(global_rows[:, None] == global_cols[None, :], parent_diag[0][:, None], 0.0)
    parent_out = my_half([own], own_map) + diagonal + my_half(sibling, partner_map)
    return (pivot_out[None], border_out[None], parent_out[None])


def solution(mesh):
    placed = (
        P("leaf", "row", "col"),
        P("leaf", "row", "col"),
        P("leaf", "row", "col"),
        P(),
        P("leaf", "row"),
    )
    return jax.shard_map(
        on_device,
        mesh=mesh,
        in_specs=placed,
        out_specs=(P("leaf", "row", "col"), P("leaf", "row", "col"), P("leaf", "row", "col")),
        check_vma=False,
    )
```
